32 devices in a mesh: dp: 2 (over x), cp: 4 (over z), tensor: 4 (over y, core).
Axes of the slice: x: 2, y: 2, z: 4, core: 2. Of those that a mesh axis runs over, the one named last changes fastest.
Arguments:
- x_in: bfloat16 [8192, 2048], P('tensor', ('dp', 'cp')), parts along dimension 1, may hold values from -6 to 6
- z_gate: bfloat16 [8192, 2048], P('tensor', ('dp', 'cp')), parts along dimension 1, may hold values from -6 to 6
- bc_in: bfloat16 [8, 256, 2048], P(None, None, ('dp', 'cp')), parts along dimension 2, may hold values from -6 to 6
- dt_raw: bfloat16 [128, 2048], P('tensor', ('dp', 'cp')), parts along dimension 1, may hold values from -3 to 13
- conv_x_w: float32 [8192, 4], P('tensor'), may hold values from -3 to 3
- conv_x_b: float32 [8192], P('tensor'), may hold values from -1.7 to 0.3
- conv_bc_w: float32 [8, 256, 4], replicated, may hold values from -3 to 3
- conv_bc_b: float32 [8, 256], replicated, may hold values from -1.7 to 0.3
- dt_bias: float32 [128], P('tensor'), may hold values from -10 to -1.5
- a_log: float32 [128], P('tensor'), may hold values from -4.6 to -2
- d_skip: float32 [128], P('tensor'), may hold values from 0.5 to 2
Outputs:
- y_out: bfloat16 [8192, 2048], P('tensor', ('dp', 'cp')), parts along dimension 1
The draws below stay inside these ranges and needn't reach their ends.
There are 2 independent parts, one for each index of `dp`. The reference program is written for one: setup_inputs(seed, part) draws one part's arguments, and reference() takes and returns one part's arrays. A program takes and returns all parts, laid end to end along the dimension named above; an argument that names none is the same for every part. Nothing has to cross between parts.
All inputs are finite; a program needn't handle non-finite values.
Results may differ from the reference program's by a relative error of at most 0.0085.
Values may be sent and summed in bfloat16 or wider, within the bound.
A program may use at most 64 MiB of HBM per device.

```python
import math
import jax
import jax.numpy as jnp
from jax import lax

HEADS = 128
HEAD_DIM = 64
STATE = 128
GROUPS = 8
KERNEL = 4
BLOCK = 256
SEQUENCE_LENGTH = 1024
CHANNELS = 8192


lift_share = 0.1875


raise_elevation = 3.8


surge_start = 1.4


def head_law(key):
    base_key = jax.random.fold_in(key, 7)
    subkeys = jax.random.split(base_key, 4)
    slow_share = 0.5
    nodes = jnp.array([-0.866, 0.0, 0.866], jnp.float32)
    node_weights = jnp.array([1.0 / 6.0, 2.0 / 3.0, 1.0 / 6.0], jnp.float32)
    is_slow = jax.random.uniform(subkeys[0], (HEADS,)) < slow_share
    spread = jax.random.uniform(subkeys[1], (HEADS,), minval=-0.2, maxval=0.2)
    slow_rate = jax.random.uniform(subkeys[2], (HEADS,), minval=0.4, maxval=0.8) / SEQUENCE_LENGTH
    fast_rate = jax.random.uniform(subkeys[3], (HEADS,), minval=1.0 / 50, maxval=1.0 / 30)
    start_delta = jnp.where(is_slow, 2.0 / SEQUENCE_LENGTH * jnp.exp(spread), 0.1 * jnp.exp(2.5 * spread))
    decay_rate = jnp.where(is_slow, slow_rate, fast_rate)
    base_raw = jnp.log(jnp.expm1(start_delta))
    drawn_mean = jnp.sum(jax.nn.softplus(base_raw[:, None] + nodes[None, :]) * node_weights[None, :], axis=1)
    lifted_mean = jnp.sum(jax.nn.softplus(base_raw[:, None] + raise_elevation + nodes[None, :]) * node_weights[None, :], axis=1)
    mean_delta = (1.0 - lift_share) * drawn_mean + lift_share * lifted_mean
    return (start_delta, decay_rate / mean_delta)


def draw_dt_bias(key, part):
    start_delta, magnitude = head_law(key)
    return jnp.log(jnp.expm1(start_delta)).astype(jnp.float32)


def draw_a_log(key, part):
    start_delta, magnitude = head_law(key)
    return jnp.log(magnitude).astype(jnp.float32)


def draw_dt_raw(key, part):
    jitter_key, lift_key, place_key, elevation_key = jax.random.split(jax.random.fold_in(key, 3), 4)
    jitter = jnp.clip(0.5 * jax.random.normal(jitter_key, (HEADS, SEQUENCE_LENGTH)), -2.5, 2.5)
    raised_values = jax.random.uniform(lift_key, (HEADS, SEQUENCE_LENGTH)) < lift_share
    stretch_width = max(1, BLOCK // 8)
    places = jax.random.randint(place_key, (3,), 0, SEQUENCE_LENGTH - stretch_width + 1)
    elevation_values = jnp.log(SEQUENCE_LENGTH / stretch_width) + surge_start + jax.random.uniform(elevation_key, (3,), minval=-0.3, maxval=0.3)
    positions = jnp.arange(SEQUENCE_LENGTH)
    contained_flag = (positions[None, :] >= places[:, None]) & (positions[None, :] < places[:, None] + stretch_width)
    surge_spans = jnp.max(jnp.where(contained_flag, elevation_values[:, None], 0.0), axis=0)
    within_surge = jnp.any(contained_flag, axis=0)
    raise_amount = jnp.where(within_surge[None, :], surge_spans[None, :], jnp.where(raised_values, raise_elevation, 0.0))
    return (jitter + raise_amount).astype(jnp.bfloat16)


def levels(stream_key, extent, shards, smallest, top_value):
    def one(axis_at, blocks):
        steps = jax.random.uniform(jax.random.fold_in(jax.random.fold_in(stream_key, 6), axis_at), (blocks,), jnp.float32, smallest / len(shards), top_value / len(shards))
        return jnp.repeat(jnp.exp(steps), extent[axis_at] // blocks).reshape((-1,) + (1,) * (len(extent) - axis_at - 1))

    level = one(*shards[0])
    for cut in shards[1:]:
        level = level * one(*cut)
    return level


def centred(rng, extent, scale, most, cuts=(), dtype=jnp.bfloat16):
    level = levels(rng, extent, cuts, -0.22, 0.18) if cuts else 1.0
    values = jax.random.normal(rng, extent, jnp.float32) * scale * level
    return jnp.minimum(jnp.maximum(values, -most), most).astype(dtype)


def setup_inputs(seed: int = 0, part: int = 0) -> dict:
    key_of = jax.random.split(jax.random.key(seed), 12)
    own_keys = jax.random.split(jax.random.fold_in(key_of[11], part), 12)
    return {
        "x_in": centred(own_keys[0], (CHANNELS, SEQUENCE_LENGTH), 1.0, 6.0, ((0, 4), (1, 4))),
        "z_gate": centred(own_keys[1], (CHANNELS, SEQUENCE_LENGTH), 1.0, 6.0, ((0, 4), (1, 4))),
        "bc_in": centred(own_keys[2], (GROUPS, 2 * STATE, SEQUENCE_LENGTH), 1.0, 6.0, ((2, 4),)),
        "dt_raw": draw_dt_raw(jax.random.fold_in(jax.random.fold_in(key_of[11], part), 71), part),
        "conv_x_w": centred(key_of[4], (CHANNELS, KERNEL), KERNEL ** -0.5, 3.0, ((0, 4),), jnp.float32),
        "conv_x_b": jnp.clip(-1.7 + 2 * jax.random.uniform(key_of[5], (CHANNELS,), jnp.float32) ** levels(key_of[5], (CHANNELS,), ((0, 4),), -0.2, 0.2), -1.7, 0.3),
        "conv_bc_w": centred(key_of[6], (GROUPS, 2 * STATE, KERNEL), KERNEL ** -0.5, 3.0, (), jnp.float32),
        "conv_bc_b": jnp.clip(jax.random.uniform(key_of[7], (GROUPS, 2 * STATE), jnp.float32, -1.7, 0.3), -1.7, 0.3),
        "dt_bias": draw_dt_bias(jax.random.fold_in(key_of[11], 71), part),
        "a_log": draw_a_log(jax.random.fold_in(key_of[11], 71), part),
        "d_skip": jnp.clip(jnp.exp(math.log(2.0) - 1.3862944 * jax.random.uniform(key_of[10], (HEADS,), jnp.float32) ** levels(key_of[10], (HEADS,), ((0, 4),), -0.2, 0.2)), 0.5, 2.0),
    }


def causal_filter(series, taps, offsets):
    kernel_size = taps.shape[-1]
    length = series.shape[-1]
    history = jnp.zeros(series.shape[:-1] + (kernel_size - 1,), jnp.float32)
    padded = jnp.concatenate([history, series], axis=-1)
    summed = jnp.broadcast_to(offsets[..., None], series.shape)
    for tap_index in range(kernel_size):
        summed = summed + taps[..., tap_index:tap_index + 1] * padded[..., tap_index:tap_index + length]
    return jax.nn.silu(summed)


def group_output(x_values, step_size, rates, skip, b_rows, c_rows):
    unit_count, channels, length = x_values.shape
    state_dim = b_rows.shape[0]
    nblocks = length // BLOCK
    cumulative = jnp.cumsum((step_size * rates[:, None]).reshape(unit_count, nblocks, BLOCK), axis=2)
    block_ends = cumulative[:, :, BLOCK - 1]
    input_gain = step_size.reshape(unit_count, nblocks, BLOCK) * jnp.exp(block_ends[:, :, None] - cumulative)
    x_wide = x_values.astype(jnp.float32)
    weighted = (x_wide.reshape(unit_count, channels, nblocks, BLOCK) * input_gain[:, None]).astype(jnp.bfloat16)
    b_wide = b_rows.astype(jnp.float32).reshape(state_dim, nblocks, BLOCK)
    c_wide = c_rows.astype(jnp.float32).reshape(state_dim, nblocks, BLOCK)
    fresh = jnp.einsum("ucbs,nbs->ubcn", weighted.astype(jnp.float32), b_wide)

    def advance(carried, inputs):
        decay, new_state = inputs
        return jnp.exp(decay)[:, None, None] * carried + new_state, carried

    unused, entering = lax.scan(advance, jnp.zeros((unit_count, channels, state_dim), jnp.float32),
                                (block_ends.T, jnp.moveaxis(fresh, 1, 0)))
    rounded = lax.optimization_barrier(entering.astype(jnp.bfloat16)).astype(jnp.float32)
    from_state = jnp.einsum("bucn,nbt->ucbt", rounded, c_wide) * jnp.exp(cumulative)[:, None]

    step_blocks = math.gcd(nblocks, max(1, 1024 // BLOCK))
    rows_step = step_blocks * BLOCK
    causal = lax.broadcasted_iota(jnp.int32, (BLOCK, BLOCK), 0) >= lax.broadcasted_iota(jnp.int32, (BLOCK, BLOCK), 1)

    def one_step(index, result):
        index = jnp.asarray(index).astype(jnp.int32)
        start = index * rows_step
        x_part = lax.dynamic_slice_in_dim(x_wide, start, rows_step, 2).reshape(unit_count, channels, step_blocks, BLOCK)
        d_part = lax.dynamic_slice_in_dim(step_size, start, rows_step, 1).reshape(unit_count, step_blocks, BLOCK)
        cum_part = lax.dynamic_slice_in_dim(cumulative, index * step_blocks, step_blocks, 1)
        b_part = lax.dynamic_slice_in_dim(b_wide, index * step_blocks, step_blocks, 1)
        c_part = lax.dynamic_slice_in_dim(c_wide, index * step_blocks, step_blocks, 1)
        gram = jnp.einsum("nbt,nbs->bts", c_part, b_part)
        spread = cum_part[:, :, :, None] - cum_part[:, :, None, :]
        decayed = jnp.where(causal, jnp.exp(jnp.where(causal, spread, 0.0)), 0.0)
        mixing = (gram[None] * decayed * d_part[:, :, None, :]).astype(jnp.bfloat16)
        mixing = lax.optimization_barrier(mixing).astype(jnp.float32)
        y_part = jnp.einsum("ucbs,ubts->ucbt", x_part, mixing)
        return lax.dynamic_update_slice_in_dim(result, y_part.reshape(unit_count, channels, rows_step), start, 2)

    intra = lax.fori_loop(0, nblocks // step_blocks, one_step,
                          jnp.zeros((unit_count, channels, length), jnp.float32))
    summed = intra + from_state.reshape(unit_count, channels, length) + skip[:, None, None] * x_wide
    return summed.astype(jnp.bfloat16)


def reference(x_in, z_gate, bc_in, dt_raw, conv_x_w, conv_x_b, conv_bc_w, conv_bc_b, dt_bias, a_log, d_skip):
    length = x_in.shape[1]
    group_heads = HEADS // GROUPS
    x_conv = causal_filter(x_in.astype(jnp.float32), conv_x_w, conv_x_b).astype(jnp.bfloat16)
    bc_conv = causal_filter(bc_in.astype(jnp.float32), conv_bc_w, conv_bc_b).astype(jnp.bfloat16)
    step_size = jax.nn.softplus(dt_raw.astype(jnp.float32) + dt_bias[:, None])
    rates = -jnp.exp(a_log)

    def group_work(operands):
        x_group, d_group, r_group, s_group, bc_group = operands
        return group_output(x_group.reshape(group_heads, HEAD_DIM, length), d_group, r_group, s_group,
                            bc_group[:STATE], bc_group[STATE:])

    mixed_out = lax.map(group_work, (x_conv.reshape(GROUPS, group_heads * HEAD_DIM, length),
                                     step_size.reshape(GROUPS, group_heads, length),
                                     rates.reshape(GROUPS, group_heads),
                                     d_skip.reshape(GROUPS, group_heads), bc_conv))
    mixed_out = lax.optimization_barrier(mixed_out.reshape(HEADS * HEAD_DIM, length))
    return (mixed_out.astype(jnp.float32) * jax.nn.silu(z_gate.astype(jnp.float32))).astype(jnp.bfloat16)
```

```python
import functools
import math

import jax
import jax.numpy as jnp
from jax import lax
from jax.experimental import pallas as pl
from jax.experimental.pallas import tpu as pltpu
from jax.sharding import PartitionSpec as P

HEADS = 128
GROUPS = 8
BLOCK = 256
LANES = 128
LOG2E = 1.4426950408889634
F32 = jnp.float32
BF16 = jnp.bfloat16


def dot(a, b, ca, cb, precision=None):
    return lax.dot_general(
        a, b, (((ca,), (cb,)), ((), ())), preferred_element_type=F32, precision=precision
    )


def silu(v):
    half = 0.5 * v
    return half + half * jnp.tanh(half)


def one_hot_rows(rows, first, kernel_size):
    r = lax.broadcasted_iota(jnp.int32, (rows, LANES), 0) - first
    lane = lax.broadcasted_iota(jnp.int32, (rows, LANES), 1)
    keep = kernel_size - 1
    hit = (r >= 0) & (r < keep) & (lane == r + LANES - keep)
    return jnp.where(hit, 1.0, 0.0).astype(BF16)


def conv_rows(values, before, columns, kernel_size):
    lane = lax.broadcasted_iota(jnp.int32, (values.shape[0], LANES), 1)
    first, second = values[:, :LANES], values[:, LANES:]
    bias = columns[:, kernel_size : kernel_size + 1]
    last = columns[:, kernel_size - 1 : kernel_size]
    out0 = bias + last * first
    out1 = bias + last * second
    for d in range(1, kernel_size):
        tap = columns[:, kernel_size - 1 - d : kernel_size - d]
        tail = lane >= LANES - d
        out0 = out0 + tap * pltpu.roll(jnp.where(tail, before, first), d, 1)
        out1 = out1 + tap * pltpu.roll(jnp.where(tail, first, second), d, 1)
    return silu(jnp.concatenate([out0, out1], axis=1)).astype(BF16)


def mixer(
    cfg,
    x_ref, bc_hbm, dt_ref, wx_ref, bx_ref, wbc_ref, bbc_ref, dtb_ref, alog_ref, dskip_ref,
    y_ref,
    bc_buf, halo_out, halo_in, wcol, xc, bcc, gram, fresh, send_buf, recv_buf,
    cum2, ecum, gain, decay, cols, acc,
    bc_sem, halo_sem, send_sem, recv_sem,
):
    n_cp, heads, hc, kernel_size, lgroups, state = cfg
    channels = x_ref.shape[0]
    head_dim = channels // heads
    rows = hc * head_dim
    chunks = heads // hc
    per_group = heads // lgroups
    me = lax.axis_index("cp")
    nxt = lax.rem(me + 1, n_cp)
    prv = lax.rem(me + n_cp - 1, n_cp)
    first_group = lax.axis_index("tensor") * heads // (HEADS // GROUPS)
    has_prev = me > 0
    has_next = me < n_cp - 1
    xblocks = channels // LANES
    bblocks = 2 * state // LANES
    hrows = halo_out.shape[0]

    bc_copy = pltpu.make_async_copy(bc_hbm.at[pl.ds(first_group, lgroups)], bc_buf, bc_sem)
    bc_copy.start()

    barrier = pltpu.get_barrier_semaphore()

    @pl.when(has_prev)
    def _():
        pl.semaphore_signal(barrier, inc=1, device_id={"cp": prv})

    @pl.when(has_next)
    def _():
        pl.semaphore_signal(barrier, inc=1, device_id={"cp": nxt})

    halo = jnp.zeros((hrows, LANES), F32)
    for b in range(xblocks):
        tail = x_ref[b * LANES : (b + 1) * LANES, BLOCK - LANES :]
        halo = halo + dot(one_hot_rows(hrows, 4 * b, kernel_size), tail, 1, 1)
    bc_copy.wait()
    for g in range(lgroups):
        for k in range(bblocks):
            tail = bc_buf[g, k * LANES : (k + 1) * LANES, BLOCK - LANES :]
            at = 4 * (xblocks + g * bblocks + k)
            halo = halo + dot(one_hot_rows(hrows, at, kernel_size), tail, 1, 1)
    halo_out[...] = halo.astype(BF16)

    pl.semaphore_wait(barrier, has_prev.astype(jnp.int32) + has_next.astype(jnp.int32))

    halo_copy = pltpu.make_async_remote_copy(
        src_ref=halo_out, dst_ref=halo_in, send_sem=halo_sem.at[0], recv_sem=halo_sem.at[1],
        device_id={"cp": nxt},
    )

    def state_copy(j):
        return pltpu.make_async_remote_copy(
            src_ref=send_buf.at[j], dst_ref=recv_buf.at[j],
            send_sem=send_sem.at[j], recv_sem=recv_sem.at[j], device_id={"cp": nxt},
        )

    @pl.when(has_next)
    def _():
        halo_copy.start()

    @pl.when(jnp.logical_not(has_prev))
    def _():
        halo_in[...] = jnp.zeros_like(halo_in)
        recv_buf[...] = jnp.zeros_like(recv_buf)

    row = lax.broadcasted_iota(jnp.int32, (heads, BLOCK), 0)
    bias = jnp.zeros((heads, BLOCK), F32)
    alog = jnp.zeros((heads, BLOCK), F32)
    for h in range(heads):
        bias = jnp.where(row == h, dtb_ref[h], bias)
        alog = jnp.where(row == h, alog_ref[h], alog)
    grown = jnp.exp(dt_ref[...].astype(F32) + bias)
    series = grown * (1.0 - grown * (0.5 - grown * (1.0 / 3.0 - 0.25 * grown)))
    delta = jnp.where(grown < 0.01, series, jnp.log(1.0 + grown))
    s_at = lax.broadcasted_iota(jnp.int32, (BLOCK, BLOCK), 0)
    t_at = lax.broadcasted_iota(jnp.int32, (BLOCK, BLOCK), 1)
    upper = jnp.where(s_at <= t_at, 1.0, 0.0)
    cum = dot(
        delta * (jnp.exp(alog) * (-LOG2E)), upper, 1, 0, precision=lax.Precision.HIGHEST
    )
    end = cum[:, BLOCK - 1 : BLOCK]
    cum2[...] = cum
    ecum[...] = jnp.exp2(cum)
    gain[...] = delta * jnp.exp2(end - cum)
    decay[...] = jnp.broadcast_to(jnp.exp2(end), (heads, LANES))
    source = jnp.transpose(jnp.log2(delta) - cum)
    for j in range(chunks):
        cols[j] = source[:, j * hc : (j + 1) * hc]

    def columns_of(taps, offsets):
        width = taps.shape[1]
        fill = jnp.zeros((8 - kernel_size - 1, width), F32)
        return jnp.transpose(jnp.concatenate([taps, offsets, fill], axis=0))

    wcol[...] = columns_of(wx_ref[...], bx_ref[...])

    @pl.when(has_prev)
    def _():
        halo_copy.wait_recv()

    def before_of(block):
        return dot(halo_in[...], one_hot_rows(hrows, 4 * block, kernel_size), 0, 0)

    for g in range(lgroups):
        columns = columns_of(wbc_ref[first_group + g], bbc_ref[pl.ds(first_group + g, 1), :])
        for k in range(bblocks):
            at = slice(k * LANES, (k + 1) * LANES)
            bcc[g, at, :] = conv_rows(
                bc_buf[g, at, :].astype(F32), before_of(xblocks + g * bblocks + k),
                columns[at], kernel_size,
            )
        gram[g] = dot(bcc[g, :state, :], bcc[g, state:, :], 0, 0)

    def spread(ref, j):
        return jnp.concatenate(
            [
                jnp.broadcast_to(ref[pl.ds(j * hc + i, 1), :], (head_dim, ref.shape[1]))
                for i in range(hc)
            ],
            axis=0,
        )

    def prepare(j, carry):
        start = pl.multiple_of(j * rows, rows)
        for b in range(rows // LANES):
            at = pl.ds(pl.multiple_of(start + b * LANES, LANES), LANES)
            xc[at, :] = conv_rows(
                x_ref[at, :].astype(F32), before_of(j * (rows // LANES) + b), wcol[at, :], kernel_size
            )
        wide = xc[pl.ds(start, rows), :].astype(F32)
        weighted = (wide * spread(gain, j)).astype(BF16)
        new = dot(weighted, bcc[j * hc // per_group, :state, :], 1, 1)
        fresh[j] = new

        @pl.when(jnp.logical_not(has_prev) & has_next)
        def _():
            send_buf[j] = new.astype(BF16)
            state_copy(j).start()

        return carry

    lax.fori_loop(0, chunks, prepare, 0)

    half_s = lax.broadcasted_iota(jnp.int32, (LANES, LANES), 0)
    half_t = lax.broadcasted_iota(jnp.int32, (LANES, LANES), 1)
    causal = half_s <= half_t
    empty = jnp.zeros((LANES, LANES), BF16)

    def finish(j, carry):
        start = pl.multiple_of(j * rows, rows)
        g = j * hc // per_group
        for i in range(hc):
            h = j * hc + i
            at = pl.ds(pl.multiple_of(start + i * head_dim, head_dim), head_dim)
            to = cum2[pl.ds(h, 1), :]
            of = cols[j, :, i : i + 1]
            near0 = jnp.where(causal, jnp.exp2(to[:, :LANES] + of[:LANES]), 0.0)
            far = jnp.exp2(to[:, LANES:] + of[:LANES])
            near1 = jnp.where(causal, jnp.exp2(to[:, LANES:] + of[LANES:]), 0.0)
            m00 = (near0 * gram[g, :LANES, :LANES]).astype(BF16)
            m01 = (far * gram[g, :LANES, LANES:]).astype(BF16)
            m11 = (near1 * gram[g, LANES:, LANES:]).astype(BF16)
            mixing = jnp.concatenate(
                [jnp.concatenate([m00, m01], axis=1), jnp.concatenate([empty, m11], axis=1)], axis=0
            )
            own = xc[at, :]
            acc[i * head_dim : (i + 1) * head_dim, :] = (
                dot(own, mixing, 1, 0) + dskip_ref[h] * own.astype(F32)
            )

        @pl.when(has_prev)
        def _():
            state_copy(j).wait_recv()

        @pl.when(has_prev & has_next)
        def _():
            passed = spread(decay, j) * recv_buf[j].astype(F32) + fresh[j]
            send_buf[j] = passed.astype(BF16)
            state_copy(j).start()

        carried = dot(recv_buf[j], bcc[g, state:, :], 1, 0)
        y_ref[pl.ds(start, rows), :] = (acc[...] + spread(ecum, j) * carried).astype(BF16)
        return carry

    lax.fori_loop(0, chunks, finish, 0)

    @pl.when(has_next)
    def _():
        halo_copy.wait_send()

        def drain(j, carry):
            state_copy(j).wait_send()
            return carry

        lax.fori_loop(0, chunks, drain, 0)


def local(
    x_in, z_gate, bc_in, dt_raw, conv_x_w, conv_x_b, conv_bc_w, conv_bc_b, dt_bias, a_log, d_skip
):
    heads = dt_raw.shape[0]
    length = dt_raw.shape[1]
    assert length == BLOCK
    channels = x_in.shape[0]
    state = bc_in.shape[1] // 2
    kernel_size = conv_x_w.shape[1]
    lgroups = max(1, heads * GROUPS // HEADS)
    hc = math.gcd(heads // lgroups, 4)
    chunks = heads // hc
    rows = channels // chunks
    n_cp = lax.axis_size("cp")
    blocks = channels // LANES + lgroups * 2 * state // LANES
    hrows = -(-4 * blocks // 16) * 16
    vmem = pl.BlockSpec(memory_space=pltpu.VMEM)
    smem = pl.BlockSpec(memory_space=pltpu.SMEM)
    y = pl.pallas_call(
        functools.partial(mixer, (n_cp, heads, hc, kernel_size, lgroups, state)),
        out_shape=jax.ShapeDtypeStruct((channels, length), BF16),
        in_specs=[vmem, pl.BlockSpec(memory_space=pl.ANY)] + [vmem] * 5 + [smem] * 3,
        out_specs=vmem,
        scratch_shapes=[
            pltpu.VMEM((lgroups, 2 * state, length), BF16),
            pltpu.VMEM((hrows, LANES), BF16),
            pltpu.VMEM((hrows, LANES), BF16),
            pltpu.VMEM((channels, 8), F32),
            pltpu.VMEM((channels, length), BF16),
            pltpu.VMEM((lgroups, 2 * state, length), BF16),
            pltpu.VMEM((lgroups, length, length), F32),
            pltpu.VMEM((chunks, rows, state), F32),
            pltpu.VMEM((chunks, rows, state), BF16),
            pltpu.VMEM((chunks, rows, state), BF16),
            pltpu.VMEM((heads, length), F32),
            pltpu.VMEM((heads, length), F32),
            pltpu.VMEM((heads, length), F32),
            pltpu.VMEM((heads, LANES), F32),
            pltpu.VMEM((chunks, length, hc), F32),
            pltpu.VMEM((rows, length), F32),
            pltpu.SemaphoreType.DMA,
            pltpu.SemaphoreType.DMA((2,)),
            pltpu.SemaphoreType.DMA((chunks,)),
            pltpu.SemaphoreType.DMA((chunks,)),
        ],
        compiler_params=pltpu.CompilerParams(
            collective_id=0, has_side_effects=True, vmem_limit_bytes=48 * 2**20
        ),
        name="mixer",
    )(
        x_in, bc_in, dt_raw, conv_x_w.T, conv_x_b[None], jnp.swapaxes(conv_bc_w, 1, 2), conv_bc_b,
        dt_bias, a_log, d_skip,
    )
    gate = z_gate.astype(F32)
    return (y.astype(F32) * jax.nn.silu(gate)).astype(BF16)


def solution(mesh):
    return jax.shard_map(
        local,
        mesh=mesh,
        in_specs=(
            P("tensor", ("dp", "cp")),
            P("tensor", ("dp", "cp")),
            P(None, None, ("dp", "cp")),
            P("tensor", ("dp", "cp")),
            P("tensor", None),
            P("tensor"),
            P(),
            P(),
            P("tensor"),
            P("tensor"),
            P("tensor"),
        ),
        out_specs=P("tensor", ("dp", "cp")),
        check_vma=False,
    )
```

```python
import functools
import math

import jax
import jax.numpy as jnp
from jax import lax
from jax.experimental import pallas as pl
from jax.experimental.pallas import tpu as pltpu
from jax.sharding import PartitionSpec as P

HEADS = 128
GROUPS = 8
BLOCK = 256
LANES = 128
LOG2E = 1.4426950408889634
F32 = jnp.float32
BF16 = jnp.bfloat16


def dot(a, b, ca, cb, precision=None):
    return lax.dot_general(
        a, b, (((ca,), (cb,)), ((), ())), preferred_element_type=F32, precision=precision
    )


def silu(v):
    half = 0.5 * v
    return half + half * jnp.tanh(half)


def one_hot_rows(rows, first, kernel_size):
    r = lax.broadcasted_iota(jnp.int32, (rows, LANES), 0) - first
    lane = lax.broadcasted_iota(jnp.int32, (rows, LANES), 1)
    keep = kernel_size - 1
    hit = (r >= 0) & (r < keep) & (lane == r + LANES - keep)
    return jnp.where(hit, 1.0, 0.0).astype(BF16)


def conv_rows(values, before, columns, kernel_size):
    lane = lax.broadcasted_iota(jnp.int32, (values.shape[0], LANES), 1)
    first, second = values[:, :LANES], values[:, LANES:]
    bias = columns[:, kernel_size : kernel_size + 1]
    last = columns[:, kernel_size - 1 : kernel_size]
    out0 = bias + last * first
    out1 = bias + last * second
    for d in range(1, kernel_size):
        tap = columns[:, kernel_size - 1 - d : kernel_size - d]
        tail = lane >= LANES - d
        out0 = out0 + tap * pltpu.roll(jnp.where(tail, before, first), d, 1)
        out1 = out1 + tap * pltpu.roll(jnp.where(tail, first, second), d, 1)
    return silu(jnp.concatenate([out0, out1], axis=1)).astype(BF16)


def mixer(
    cfg,
    x_hbm, bc_hbm, dt_hbm, wx_hbm, bx_hbm, wbc_hbm, bbc_hbm, dtb_hbm, alog_hbm, dskip_hbm,
    y_ref,
    x_ref, dt_ref, wx_ref, bx_ref, wbc_ref, bbc_ref, dtb_ref, alog_ref, dskip_ref,
    bc_buf, halo_out, halo_in, wcol, xc, bcc, gram, fresh, send_buf, recv_buf,
    cum2, ecum, gain, decay, skip, cols, acc,
    in_sem, bc_sem, halo_sem, send_sem, recv_sem,
):
    n_cp, heads, hc, kernel_size, lgroups, state = cfg
    channels = x_ref.shape[0]
    head_dim = channels // heads
    rows = hc * head_dim
    chunks = heads // hc
    per_group = heads // lgroups
    me = lax.axis_index("cp")
    nxt = lax.rem(me + 1, n_cp)
    prv = lax.rem(me + n_cp - 1, n_cp)
    first_group = lax.axis_index("tensor") * heads // (HEADS // GROUPS)
    has_prev = me > 0
    has_next = me < n_cp - 1
    xblocks = channels // LANES
    bblocks = 2 * state // LANES
    hrows = halo_out.shape[0]

    bc_copy = pltpu.make_async_copy(bc_hbm.at[pl.ds(first_group, lgroups)], bc_buf, bc_sem)
    bc_copy.start()

    right, left = pl.ds(BLOCK - LANES, LANES), pl.ds(0, LANES)
    pairs = (
        (x_hbm.at[:, right], x_ref.at[:, right]),
        (dt_hbm, dt_ref), (dtb_hbm, dtb_ref), (alog_hbm, alog_ref), (dskip_hbm, dskip_ref),
        (wx_hbm, wx_ref), (bx_hbm, bx_ref),
        (wbc_hbm.at[pl.ds(first_group, lgroups)], wbc_ref), (bbc_hbm, bbc_ref),
        (x_hbm.at[:, left], x_ref.at[:, left]),
    )
    loads = [
        pltpu.make_async_copy(src, dst, in_sem.at[i]) for i, (src, dst) in enumerate(pairs)
    ]
    for load in loads:
        load.start()

    barrier = pltpu.get_barrier_semaphore()

    @pl.when(has_prev)
    def _():
        pl.semaphore_signal(barrier, inc=1, device_id={"cp": prv})

    @pl.when(has_next)
    def _():
        pl.semaphore_signal(barrier, inc=1, device_id={"cp": nxt})

    halo = jnp.zeros((hrows, LANES), F32)
    loads[0].wait()
    for b in range(xblocks):
        tail = x_ref[b * LANES : (b + 1) * LANES, BLOCK - LANES :]
        halo = halo + dot(one_hot_rows(hrows, 4 * b, kernel_size), tail, 1, 1)
    bc_copy.wait()
    for g in range(lgroups):
        for k in range(bblocks):
            tail = bc_buf[g, k * LANES : (k + 1) * LANES, BLOCK - LANES :]
            at = 4 * (xblocks + g * bblocks + k)
            halo = halo + dot(one_hot_rows(hrows, at, kernel_size), tail, 1, 1)
    halo_out[...] = halo.astype(BF16)

    pl.semaphore_wait(barrier, has_prev.astype(jnp.int32) + has_next.astype(jnp.int32))

    halo_copy = pltpu.make_async_remote_copy(
        src_ref=halo_out, dst_ref=halo_in, send_sem=halo_sem.at[0], recv_sem=halo_sem.at[1],
        device_id={"cp": nxt},
    )

    def state_copy(j):
        return pltpu.make_async_remote_copy(
            src_ref=send_buf.at[j], dst_ref=recv_buf.at[j],
            send_sem=send_sem.at[j], recv_sem=recv_sem.at[j], device_id={"cp": nxt},
        )

    @pl.when(has_next)
    def _():
        halo_copy.start()

    @pl.when(jnp.logical_not(has_prev))
    def _():
        halo_in[...] = jnp.zeros_like(halo_in)
        recv_buf[...] = jnp.zeros_like(recv_buf)

    for load in loads[1:]:
        load.wait()
    vectors = jnp.transpose(
        jnp.concatenate(
            [dtb_ref[...], alog_ref[...], dskip_ref[...], jnp.zeros((5, heads), F32)], axis=0
        )
    )
    bias = vectors[:, 0:1]
    alog = vectors[:, 1:2]
    skip[...] = jnp.broadcast_to(vectors[:, 2:3], (heads, BLOCK))
    grown = jnp.exp(dt_ref[...].astype(F32) + bias)
    series = grown * (1.0 - grown * (0.5 - grown * (1.0 / 3.0 - 0.25 * grown)))
    delta = jnp.where(grown < 0.01, series, jnp.log(1.0 + grown))
    s_at = lax.broadcasted_iota(jnp.int32, (BLOCK, BLOCK), 0)
    t_at = lax.broadcasted_iota(jnp.int32, (BLOCK, BLOCK), 1)
    upper = jnp.where(s_at <= t_at, 1.0, 0.0)
    cum = dot(
        delta * (jnp.exp(alog) * (-LOG2E)), upper, 1, 0, precision=lax.Precision.HIGHEST
    )
    end = cum[:, BLOCK - 1 : BLOCK]
    cum2[...] = cum
    ecum[...] = jnp.exp2(cum)
    gain[...] = delta * jnp.exp2(end - cum)
    decay[...] = jnp.broadcast_to(jnp.exp2(end), (heads, LANES))
    source = jnp.transpose(jnp.log2(delta) - cum)
    for j in range(chunks):
        cols[j] = source[:, j * hc : (j + 1) * hc]

    def columns_of(taps, offsets):
        width = taps.shape[1]
        fill = jnp.zeros((8 - kernel_size - 1, width), F32)
        return jnp.transpose(jnp.concatenate([taps, offsets, fill], axis=0))

    wcol[...] = columns_of(wx_ref[...], bx_ref[...])

    @pl.when(has_prev)
    def _():
        halo_copy.wait_recv()

    def before_of(block):
        return dot(halo_in[...], one_hot_rows(hrows, 4 * block, kernel_size), 0, 0)

    for g in range(lgroups):
        columns = columns_of(wbc_ref[g], bbc_ref[pl.ds(first_group + g, 1), :])
        for k in range(bblocks):
            at = slice(k * LANES, (k + 1) * LANES)
            bcc[g, at, :] = conv_rows(
                bc_buf[g, at, :].astype(F32), before_of(xblocks + g * bblocks + k),
                columns[at], kernel_size,
            )
        gram[g] = dot(bcc[g, :state, :], bcc[g, state:, :], 0, 0)

    def spread(ref, j):
        return jnp.concatenate(
            [
                jnp.broadcast_to(ref[pl.ds(j * hc + i, 1), :], (head_dim, ref.shape[1]))
                for i in range(hc)
            ],
            axis=0,
        )

    def prepare(j, carry):
        start = pl.multiple_of(j * rows, rows)
        for b in range(rows // LANES):
            at = pl.ds(pl.multiple_of(start + b * LANES, LANES), LANES)
            xc[at, :] = conv_rows(
                x_ref[at, :].astype(F32), before_of(j * (rows // LANES) + b), wcol[at, :], kernel_size
            )
        wide = xc[pl.ds(start, rows), :].astype(F32)
        weighted = (wide * spread(gain, j)).astype(BF16)
        new = dot(weighted, bcc[j * hc // per_group, :state, :], 1, 1)
        fresh[j] = new

        @pl.when(jnp.logical_not(has_prev) & has_next)
        def _():
            send_buf[j] = new.astype(BF16)
            state_copy(j).start()

        return carry

    lax.fori_loop(0, chunks, prepare, 0)

    half_s = lax.broadcasted_iota(jnp.int32, (LANES, LANES), 0)
    half_t = lax.broadcasted_iota(jnp.int32, (LANES, LANES), 1)
    causal = half_s <= half_t
    empty = jnp.zeros((LANES, LANES), BF16)

    def finish(j, carry):
        start = pl.multiple_of(j * rows, rows)
        g = j * hc // per_group
        for i in range(hc):
            h = j * hc + i
            at = pl.ds(pl.multiple_of(start + i * head_dim, head_dim), head_dim)
            to = cum2[pl.ds(h, 1), :]
            of = cols[j, :, i : i + 1]
            near0 = jnp.where(causal, jnp.exp2(to[:, :LANES] + of[:LANES]), 0.0)
            far = jnp.exp2(to[:, LANES:] + of[:LANES])
            near1 = jnp.where(causal, jnp.exp2(to[:, LANES:] + of[LANES:]), 0.0)
            m00 = (near0 * gram[g, :LANES, :LANES]).astype(BF16)
            m01 = (far * gram[g, :LANES, LANES:]).astype(BF16)
            m11 = (near1 * gram[g, LANES:, LANES:]).astype(BF16)
            mixing = jnp.concatenate(
                [jnp.concatenate([m00, m01], axis=1), jnp.concatenate([empty, m11], axis=1)], axis=0
            )
            own = xc[at, :]
            acc[i * head_dim : (i + 1) * head_dim, :] = (
                dot(own, mixing, 1, 0) + skip[pl.ds(h, 1), :] * own.astype(F32)
            )

        @pl.when(has_prev)
        def _():
            state_copy(j).wait_recv()

        @pl.when(has_prev & has_next)
        def _():
            passed = spread(decay, j) * recv_buf[j].astype(F32) + fresh[j]
            send_buf[j] = passed.astype(BF16)
            state_copy(j).start()

        carried = dot(recv_buf[j], bcc[g, state:, :], 1, 0)
        y_ref[pl.ds(start, rows), :] = (acc[...] + spread(ecum, j) * carried).astype(BF16)
        return carry

    lax.fori_loop(0, chunks, finish, 0)

    @pl.when(has_next)
    def _():
        halo_copy.wait_send()

        def drain(j, carry):
            state_copy(j).wait_send()
            return carry

        lax.fori_loop(0, chunks, drain, 0)


def local(
    x_in, z_gate, bc_in, dt_raw, conv_x_w, conv_x_b, conv_bc_w, conv_bc_b, dt_bias, a_log, d_skip
):
    heads = dt_raw.shape[0]
    length = dt_raw.shape[1]
    assert length == BLOCK
    channels = x_in.shape[0]
    state = bc_in.shape[1] // 2
    kernel_size = conv_x_w.shape[1]
    lgroups = max(1, heads * GROUPS // HEADS)
    hc = math.gcd(heads // lgroups, 2)
    chunks = heads // hc
    rows = channels // chunks
    n_cp = lax.axis_size("cp")
    blocks = channels // LANES + lgroups * 2 * state // LANES
    hrows = -(-4 * blocks // 16) * 16
    vmem = pl.BlockSpec(memory_space=pltpu.VMEM)
    hbm = pl.BlockSpec(memory_space=pltpu.HBM)
    y = pl.pallas_call(
        functools.partial(mixer, (n_cp, heads, hc, kernel_size, lgroups, state)),
        out_shape=jax.ShapeDtypeStruct((channels, length), BF16),
        in_specs=[hbm] * 10,
        out_specs=vmem,
        scratch_shapes=[
            pltpu.VMEM(x_in.shape, BF16),
            pltpu.VMEM(dt_raw.shape, BF16),
            pltpu.VMEM((kernel_size, channels), F32),
            pltpu.VMEM((1, channels), F32),
            pltpu.VMEM((lgroups, kernel_size, 2 * state), F32),
            pltpu.VMEM(conv_bc_b.shape, F32),
            pltpu.VMEM((1, heads), F32),
            pltpu.VMEM((1, heads), F32),
            pltpu.VMEM((1, heads), F32),
            pltpu.VMEM((lgroups, 2 * state, length), BF16),
            pltpu.VMEM((hrows, LANES), BF16),
            pltpu.VMEM((hrows, LANES), BF16),
            pltpu.VMEM((channels, 8), F32),
            pltpu.VMEM((channels, length), BF16),
            pltpu.VMEM((lgroups, 2 * state, length), BF16),
            pltpu.VMEM((lgroups, length, length), F32),
            pltpu.VMEM((chunks, rows, state), F32),
            pltpu.VMEM((chunks, rows, state), BF16),
            pltpu.VMEM((chunks, rows, state), BF16),
            pltpu.VMEM((heads, length), F32),
            pltpu.VMEM((heads, length), F32),
            pltpu.VMEM((heads, length), F32),
            pltpu.VMEM((heads, LANES), F32),
            pltpu.VMEM((heads, length), F32),
            pltpu.VMEM((chunks, length, hc), F32),
            pltpu.VMEM((rows, length), F32),
            pltpu.SemaphoreType.DMA((10,)),
            pltpu.SemaphoreType.DMA,
            pltpu.SemaphoreType.DMA((2,)),
            pltpu.SemaphoreType.DMA((chunks,)),
            pltpu.SemaphoreType.DMA((chunks,)),
        ],
        compiler_params=pltpu.CompilerParams(
            collective_id=0, has_side_effects=True, vmem_limit_bytes=60 * 1024 * 1024
        ),
        name="mixer",
    )(
        x_in, bc_in, dt_raw, conv_x_w.T, conv_x_b[None], jnp.swapaxes(conv_bc_w, 1, 2), conv_bc_b,
        dt_bias[None], a_log[None], d_skip[None],
    )
    gate = z_gate.astype(F32)
    return (y.astype(F32) * jax.nn.silu(gate)).astype(BF16)


def solution(mesh):
    return jax.shard_map(
        local,
        mesh=mesh,
        in_specs=(
            P("tensor", ("dp", "cp")),
            P("tensor", ("dp", "cp")),
            P(None, None, ("dp", "cp")),
            P("tensor", ("dp", "cp")),
            P("tensor", None),
            P("tensor"),
            P(),
            P(),
            P("tensor"),
            P("tensor"),
            P("tensor"),
        ),
        out_specs=P("tensor", ("dp", "cp")),
        check_vma=False,
    )
```
